128 devices in a mesh: grp: 4 (over z_hi, core), row: 4 (over y), col: 8 (over x, z_lo).
Axes of the slice: x: 4, y: 4, z: 4 (z_hi: 2, z_lo: 2; z = z_hi * 2 + z_lo), core: 2. Of those that a mesh axis runs over, the one named last changes fastest.
Arguments:
- tokens: bfloat16 [8192, 4608], P(('grp', 'row', 'col')), parts along dimension 0, may hold values from -6 to 6
- ln_gain: float32 [4608], replicated, may hold values from 0.1 to 1.9
- w_in: bfloat16 [4608, 12288], P('row', 'col'), may hold values from -0.09375 to 0.09375
- b_in: float32 [12288], P('col'), may hold values from -3 to 3
- w_out: bfloat16 [12288, 4608], P('col', 'row'), may hold values from -0.0546875 to 0.0546875
- b_out: float32 [4608], P('row'), may hold values from -3 to 3
Outputs:
- result: bfloat16 [8192, 4608], P(('grp', 'row', 'col')), parts along dimension 0
The draws below stay inside these ranges and needn't reach their ends.
There are 4 independent parts, one for each index of `grp`. The reference program is written for one: setup_inputs(seed, part) draws one part's arguments, and reference() takes and returns one part's arrays. A program takes and returns all parts, laid end to end along the dimension named above; an argument that names none is the same for every part. Nothing has to cross between parts.
All inputs are finite; a program needn't handle non-finite values.
Results may differ from the reference program's by a relative error of at most 0.0095.
Values may be sent and summed in bfloat16 or wider, within the bound.
A program may use at most 128 MiB of HBM per device.

```python
import jax
import jax.numpy as jnp
from jax import lax

D = 4608
FF = 12288
TOKENS = 2048


def block_scale(own_key, dims, pieces, low, top_value):
    def one(position, blocks):
        heights = jax.random.uniform(jax.random.fold_in(jax.random.fold_in(own_key, 6), position), (blocks,), jnp.float32, low / len(pieces), top_value / len(pieces))
        return jnp.repeat(jnp.exp(heights), dims[position] // blocks).reshape((-1,) + (1,) * (len(dims) - position - 1))

    loudness = one(*pieces[0])
    for cut in pieces[1:]:
        loudness = loudness * one(*cut)
    return loudness


def normal_values(rng, shape, width, limit, shards=(), held_as=jnp.bfloat16):
    drawn = width * jax.random.normal(rng, shape, jnp.float32)
    if shards:
        drawn = drawn * block_scale(rng, shape, shards, -0.22, 0.18)
    return jnp.clip(drawn, -limit, limit).astype(held_as)


def setup_inputs(seed: int = 0, part: int = 0) -> dict:
    key_list = jax.random.split(jax.random.key(seed), 7)
    own_keys = jax.random.split(jax.random.fold_in(key_list[6], part), 7)
    tokens = normal_values(own_keys[0], (TOKENS, D), 1.0, 6.0, ((0, 32),))
    ln_gain = jnp.clip(1.0 + 0.18 * jax.random.normal(key_list[1], (D,), jnp.float32), 0.1, 1.9)
    w_in = normal_values(key_list[2], (D, FF), D ** -0.5, 0.09375, ((0, 4), (1, 8)))
    b_in = normal_values(key_list[3], (FF,), 0.5, 3.0, ((0, 8),), jnp.float32)
    w_out = normal_values(key_list[4], (FF, D), FF ** -0.5, 0.0546875, ((0, 8), (1, 4)))
    b_out = normal_values(key_list[5], (D,), 0.5, 3.0, ((0, 4),), jnp.float32)
    return {"tokens": tokens, "ln_gain": ln_gain, "w_in": w_in, "b_in": b_in, "w_out": w_out, "b_out": b_out}


def reference(tokens, ln_gain, w_in, b_in, w_out, b_out):
    values = tokens.astype(jnp.float32)
    row_mean = lax.optimization_barrier(jnp.mean(values, axis=1, keepdims=True))
    centered = values - row_mean
    row_var = lax.optimization_barrier(jnp.mean(centered * centered, axis=1, keepdims=True))
    normed = (centered * jax.lax.rsqrt(row_var + 1e-06) * ln_gain).astype(jnp.bfloat16)
    preact = jnp.dot(normed, w_in, preferred_element_type=jnp.float32) + b_in
    hidden = jax.nn.gelu(preact, approximate=False).astype(jnp.bfloat16)
    branch_out = (jnp.dot(hidden, w_out, preferred_element_type=jnp.float32) + b_out).astype(jnp.bfloat16)
    return (values + branch_out.astype(jnp.float32)).astype(jnp.bfloat16)
```

```python
import functools

import jax
import jax.numpy as jnp
from jax import lax
from jax.experimental import pallas as pl
from jax.experimental.pallas import tpu as pltpu
from jax.sharding import PartitionSpec as P

MESH = pl.DeviceIdType.MESH
F32, BF16 = jnp.float32, jnp.bfloat16
NQ = 4
N_RECV = 155
SQRT_HALF = 0.7071067811865476
OWN, UP, DOWN, FAR = 0, 1, 2, 3
C1 = 128
W1_CHUNKS = ((0, 1, 2), (1, 1, 4), (2, 2, 2), (4, 2, 4), (6, 2, 2), (8, 2, 4), (10, 2, 4))
NW2 = 9
Z = (0, 2)
OWN01, NEAR0, FAR0 = ((0, 1), (0, 2), Z), ((1, 3), (0, 1), Z), ((3, 4), (0, 1), Z)
REST0, REST1, REST2 = ((1, 4), (0, 1), Z), ((1, 4), (1, 2), Z), ((1, 4), (2, 3), Z)
NEAR3, FAR3 = ((1, 3), (3, 4), Z), ((3, 4), (3, 4), Z)
OWN23, OWN23Z1, OWN23Z0 = ((0, 1), (2, 4), Z), ((0, 1), (2, 4), (1, 2)), ((0, 1), (2, 4), (0, 1))


def kernel(dims, tok_hbm, gain_hbm, w1_hbm, b1_hbm, w2_hbm, b2_hbm, out,
           tok, gain, b1, b2_own, w1, w2, x, nb, p32, ps, pr, hid, os_, r1, r2, zs, zr, fs, fr, b2_far,
           send_sems, recv_sems, local_sems):
    tq, kb, nf = dims
    nx = 4
    width = nx * kb

    grp, y, col = lax.axis_index("grp"), lax.axis_index("row"), lax.axis_index("col")
    xx, z, core, half = col // 2, col % 2, grp % 2, grp // 2
    m = y % 2
    y_pair = y + 1 - 2 * m
    y_far = 3 - y
    x_up, x_dn = (xx + 1) % 4, (xx + 3) % 4
    core_grp = grp + 1 - 2 * core
    twin_grp = grp + 2 - 4 * half
    diag_grp = core_grp + 2 - 4 * half
    DEV = {
        "pair": (grp, y_pair, col),
        "far": (grp, y_far, col),
        "core": (core_grp, y, col),
        "twin": (twin_grp, y, col),
        "up": (grp, y, x_up * 2 + z),
        "dn": (grp, y, x_dn * 2 + z),
        "z": (grp, y, xx * 2 + 1 - z),
    }
    my_blocks = (y, y_far)
    pair_blocks = (y_pair, 3 - y_pair)

    def lanes(block):
        return pl.ds(pl.multiple_of(block * kb, 128), kb)

    ids, landing, waited, groups = {}, {}, set(), {}

    def send(key, src, dst, to, landed=None, group=None):
        i = ids.setdefault(key, len(ids))
        g = groups.setdefault(group or key[0], len(groups))
        landing[key] = (dst if landed is None else landed, to, i)
        pltpu.make_async_remote_copy(
            src_ref=src, dst_ref=dst, send_sem=send_sems.at[g], recv_sem=recv_sems.at[i],
            device_id=DEV[to], device_id_type=MESH).start()

    def need(*keys):
        for key in keys:
            if key not in waited:
                waited.add(key)
                ref, to, i = landing[key]
                pltpu.make_async_remote_copy(
                    src_ref=ref, dst_ref=ref, send_sem=send_sems.at[0], recv_sem=recv_sems.at[i],
                    device_id=DEV[to], device_id_type=MESH).wait_recv()

    def all_sent(group, ref):
        pltpu.make_async_remote_copy(
            src_ref=ref, dst_ref=ref, send_sem=send_sems.at[groups.pop(group)], recv_sem=recv_sems.at[0],
            device_id=DEV["pair"], device_id_type=MESH).wait_send()

    load_tok = pltpu.make_async_copy(tok_hbm, tok, local_sems.at[2])
    load_tok.start()
    vectors = [
        pltpu.make_async_copy(src, dst, local_sems.at[4 + i])
        for i, (src, dst) in enumerate(((gain_hbm, gain), (b1_hbm, b1), (b2_hbm, b2_own)))]
    for copy in vectors:
        copy.start()
    load1 = pltpu.make_async_copy(w1_hbm, w1.at[pl.ds(0, kb)], local_sems.at[0])
    load1.start()
    barrier = pltpu.get_barrier_semaphore()
    for to in DEV:
        pl.semaphore_signal(barrier, inc=1, device_id=DEV[to], device_id_type=MESH)

    C2 = kb // 3
    load2 = pltpu.make_async_copy(w2_hbm, w2.at[0], local_sems.at[1])
    CHUNKS = [(1, c) for c in range(len(W1_CHUNKS))] + [(2, c) for c in range(NW2)]

    def split(which, c):
        return W1_CHUNKS[c][2] if which == 1 else 4

    def part(which, c, ref, owner_grp, base=0):
        n = split(which, c)
        owner = owner_grp if n == 4 else owner_grp % 2
        if which == 1:
            c0, width1, _ = W1_CHUNKS[c]
            size, cols = kb // n, pl.ds(c0 * C1, width1 * C1)
        else:
            size, cols = nf // n, pl.ds(c * (kb // NW2), kb // NW2)
        return ref.at[pl.ds(pl.multiple_of(base + owner * size, 32), size), cols]

    def far_part(which, c, owner):
        return part(which, c, w1, owner, kb) if which == 1 else part(which, c, w2.at[1], owner)

    def send_weights():
        for which, c in CHUNKS:
            src = part(which, c, w1_hbm if which == 1 else w2_hbm, grp)
            send(("wy", which, c), src, far_part(which, c, grp), "far", group=(which, split(which, c)))
        send(("b2",), b2_hbm, b2_far, "far")
        load2.start()

    def w_y(which, c):
        mine = far_part(which, c, grp)
        group = (which, split(which, c))
        need(("wy", which, c))
        if group[1] == 4:
            send(("wt", which, c), mine, mine, "twin", far_part(which, c, twin_grp), group)
        send(("wc", which, c), mine, mine, "core", far_part(which, c, core_grp), group)

    def w_t(which, c):
        theirs = far_part(which, c, twin_grp)
        need(("wt", which, c))
        send(("wd", which, c), theirs, theirs, "core", far_part(which, c, diag_grp), (which, 4))

    def w_all(which, c):
        need(("wy", which, c), ("wc", which, c))
        if split(which, c) == 4:
            need(("wt", which, c), ("wd", which, c))

    def half_rows(mi):
        return pl.ds(pl.multiple_of(mi * tq, tq), tq)

    def norm(q):
        rows = pl.ds(q * tq, tq)
        total = jnp.zeros((tq, 1), F32)
        for b in range(nx):
            total += jnp.sum(tok[rows, pl.ds(b * kb, kb)].astype(F32), axis=1, keepdims=True)
        mean = total / width
        sq = jnp.zeros((tq, 1), F32)
        for b in range(nx):
            d = tok[rows, pl.ds(b * kb, kb)].astype(F32) - mean
            sq += jnp.sum(d * d, axis=1, keepdims=True)
        scale = lax.rsqrt(sq / width + 1e-06)

        def normed(block):
            g = gain[lanes(block)].reshape(1, kb)
            return ((tok[rows, lanes(block)].astype(F32) - mean) * scale * g).astype(BF16)

        for i, block in enumerate(pair_blocks):
            nb[rows, pl.ds(i * kb, kb)] = normed(block)
        for i, block in enumerate(my_blocks):
            x[OWN, q, 0, half_rows(m), pl.ds(i * kb, kb)] = normed(block)

    def ag_y(q):
        there = x.at[OWN, q, 0, half_rows(m)]
        send(("a2a", q), nb.at[pl.ds(q * tq, tq)], there, "pair", x.at[OWN, q, 0, half_rows(1 - m)])

    def ag_rows(q, r):
        send(("agu0", q), x.at[OWN, q, 0, r], x.at[DOWN, q, 0, r], "up", x.at[DOWN, q, 0], "ag")
        send(("agd0", q), x.at[OWN, q, 0, r], x.at[UP, q, 0, r], "dn", x.at[UP, q, 0], "ag")

    def ag_x00(q):
        ag_rows(q, half_rows(m))

    def ag_z(q):
        need(("a2a", q))
        send(("agz", q), x.at[OWN, q, 0], x.at[OWN, q, 1], "z")

    def ag_x0(q):
        need(("a2a", q))
        ag_rows(q, half_rows(1 - m))

    def ag_x1(q):
        need(("agz", q))
        send(("agu1", q), x.at[OWN, q, 1], x.at[DOWN, q, 1], "up", group="ag")
        send(("agd1", q), x.at[OWN, q, 1], x.at[UP, q, 1], "dn", group="ag")

    def ag_fu(q):
        need(("agu0", q))
        send(("agf", q), x.at[DOWN, q, 0], x.at[FAR, q, 0], "up", x.at[FAR, q])

    def ag_fd(q):
        need(("agd1", q))
        send(("agf", q), x.at[UP, q, 1], x.at[FAR, q, 1], "dn", x.at[FAR, q])

    SOURCES = {
        (OWN, 0): "a2a", (OWN, 1): "agz", (UP, 0): "agd0", (UP, 1): "agd1",
        (DOWN, 0): "agu0", (DOWN, 1): "agu1", (FAR, 0): "agf", (FAR, 1): "agf",
    }

    def at(ref, unit, cols):
        (xa, xb), (qa, qb), (za, zb) = unit
        return ref.at[pl.ds(xa, xb - xa), pl.ds(qa, qb - qa), pl.ds(za, zb - za), :, cols]

    def blocks(unit):
        (xa, xb), (qa, qb), (za, zb) = unit
        return [(i, j, k) for i in range(xa, xb) for j in range(qa, qb) for k in range(za, zb)]

    def shape_of(unit):
        (xa, xb), (qa, qb), (za, zb) = unit
        return (xb - xa, qb - qa, zb - za, 2 * tq)

    def flat(ref, unit):
        v = at(ref, unit, slice(None))[...]
        return v.reshape(-1, v.shape[-1])

    def mm1(unit, c0, n):
        if not waited & {"w1"}:
            waited.add("w1")
            load1.wait()
        for i, j, k in blocks(unit):
            need((SOURCES[i, k], j))
        for c, (first, count, _) in enumerate(W1_CHUNKS):
            if first < c0 + n and c0 < first + count:
                w_all(1, c)
        wide = C1 * (2 - n % 2)

        @pl.loop(0, n * C1 // wide)
        def _(c):
            cols = pl.ds(pl.multiple_of(c0 * C1 + c * wide, C1), wide)
            acc = jnp.dot(flat(x, unit), w1[:, cols], preferred_element_type=F32)
            acc = acc.reshape(shape_of(unit) + (wide,))
            at(p32, unit, cols)[...] = acc
            at(ps, unit, cols)[...] = acc.astype(BF16)

        cols = pl.ds(c0 * C1, n * C1)
        send(("p", unit, c0), at(ps, unit, cols), at(pr, unit, cols), "pair")

    def act(unit, c0, n):
        need(("p", unit, c0))

        @pl.loop(c0, c0 + n)
        def _(c):
            cols = pl.ds(pl.multiple_of(c * C1, C1), C1)
            bias = b1[cols].reshape(1, C1)
            for i, j, k in blocks(unit):
                v = p32[i, j, k, :, cols] + pr[i, j, k, :, cols].astype(F32) + bias
                hid[i, j, k, :, cols] = (0.5 * v * (1.0 + lax.erf(v * SQRT_HALF))).astype(BF16)

    def mm2(unit, h):
        if not waited & {"w2"}:
            waited.add("w2")
            load2.wait()
        if h:
            for c in range(NW2):
                w_all(2, c)

        @pl.loop(0, 3)
        def _(c):
            cols = pl.ds(pl.multiple_of(c * C2, 128), C2)
            acc = jnp.dot(flat(hid, unit), w2[h, :, cols], preferred_element_type=F32)
            at(os_.at[h], unit, cols)[...] = acc.reshape(shape_of(unit) + (C2,)).astype(BF16)

    def rs1(q, h):
        send(("r1", q, h), os_.at[h, FAR, q, 0], r1.at[h, q, 0], "up", r1.at[h, q])
        send(("r1", q, h), os_.at[h, FAR, q, 1], r1.at[h, q, 1], "dn", r1.at[h, q])

    def r2_send(q, h, x_pos, z_pos, to):
        d = 0 if to == "up" else 1
        send(("r2", q, h, z_pos), os_.at[h, x_pos, q, z_pos], r2.at[h, q, z_pos, d], to, r2.at[h, q, z_pos])

    def rs1n(q, h):
        r2_send(q, h, UP, 1, "up")

    def rs2(q, h):
        need(("r1", q, h))
        os_[h, UP, q, 0] = (os_[h, UP, q, 0].astype(F32) + r1[h, q, 0].astype(F32)).astype(BF16)
        r2_send(q, h, UP, 0, "up")
        os_[h, DOWN, q, 1] = (os_[h, DOWN, q, 1].astype(F32) + r1[h, q, 1].astype(F32)).astype(BF16)
        r2_send(q, h, DOWN, 1, "dn")
        r2_send(q, h, DOWN, 0, "dn")

    def rs3(q, h):
        need(("r2", q, h, 1))
        s = os_[h, OWN, q, 1].astype(F32) + r2[h, q, 1, 0].astype(F32) + r2[h, q, 1, 1].astype(F32)
        zs[h, q] = s.astype(BF16)
        send(("rz", q, h), zs.at[h, q], zr.at[h, q], "z")

    def rs4(q, h):
        rows = pl.ds(q * tq, tq)
        need(("r2", q, h, 0), ("rz", q, h))
        if h:
            need(("b2",))
        bias = (b2_far if h else b2_own)[...].reshape(1, kb)

        def branch(mi):
            r = half_rows(mi)
            s = os_[h, OWN, q, 0, r].astype(F32) + r2[h, q, 0, 0, r].astype(F32) + r2[h, q, 0, 1, r].astype(F32)
            return (s + zr[h, q, r].astype(F32) + bias).astype(BF16)

        fs[h, rows, :] = branch(1 - m)
        there = out.at[rows, lanes(my_blocks[h])]
        send(("f",), fs.at[h, rows], there, "pair", fs)
        fr[h, rows, :] = branch(m)
        pltpu.make_async_copy(fr.at[h, rows], there, local_sems.at[3]).start()

    order = [
        (ag_y, 0), (ag_x00, 3), (ag_y, 3), (ag_x00, 1), (ag_y, 1), (ag_z, 0), (ag_x00, 0), (ag_x0, 0), (ag_z, 1),
        (w_y, 1, 0), (ag_y, 2), (ag_x0, 1), (w_y, 1, 1), (ag_x1, 0), (ag_z, 2), (mm1, OWN01, 0, 1), (ag_fu, 0), (ag_x1, 1),
        (ag_fu, 1), (ag_z, 3), (w_t, 1, 1), (w_y, 1, 2), (mm1, NEAR0, 0, 1), (ag_fd, 0), (mm1, NEAR0, 1, 1),
        (mm1, OWN01, 1, 1), (ag_fd, 1), (mm1, NEAR0, 2, 2), (w_y, 1, 3), (mm1, OWN01, 2, 2), (mm1, FAR0, 1, 1),
        (mm1, OWN23, 0, 1), (mm1, OWN23, 2, 2), (ag_x00, 2), (mm1, FAR0, 0, 1), (mm1, OWN23, 1, 1), (ag_x0, 3),
        (mm1, REST1, 0, 4), (w_y, 1, 4), (ag_x0, 2), (ag_x1, 2), (w_t, 1, 3), (w_y, 1, 5), (mm1, REST1, 4, 4),
        (mm1, NEAR0, 4, 2), (ag_x1, 3), (w_y, 1, 6), (mm1, FAR0, 2, 2), (w_y, 2, 0), (mm1, FAR0, 6, 2), (w_t, 1, 5),
        (w_y, 2, 1), (ag_fd, 2), (act, OWN01, 1, 1), (ag_fu, 3), (ag_fd, 3), (mm1, NEAR0, 6, 2), (mm1, NEAR0, 8, 2),
        (w_t, 1, 6), (mm1, FAR0, 8, 2), (ag_fu, 2), (mm1, FAR0, 4, 2), (w_y, 2, 2), (act, FAR0, 1, 1), (w_y, 2, 3),
        (act, FAR0, 2, 2), (mm1, REST1, 8, 4), (mm1, NEAR0, 10, 2), (act, FAR0, 0, 1), (act, FAR0, 6, 2),
        (act, REST1, 0, 4), (act, NEAR0, 4, 2), (act, NEAR0, 1, 1), (w_y, 2, 4), (mm1, FAR0, 10, 2), (act, OWN01, 2, 2),
        (mm1, REST2, 6, 6), (act, NEAR0, 8, 2), (w_y, 2, 5), (w_y, 2, 6), (act, REST1, 4, 4), (act, FAR0, 4, 2),
        (mm1, REST2, 0, 6), (act, NEAR0, 6, 2), (act, FAR0, 8, 2), (act, NEAR0, 2, 2), (act, REST1, 8, 4), (w_t, 2, 4),
        (w_y, 2, 7), (mm2, REST1, 0), (act, NEAR0, 10, 2), (rs1, 1, 0), (act, NEAR0, 0, 1), (act, FAR0, 10, 2),
        (mm1, OWN01, 10, 2), (w_y, 2, 8), (w_t, 2, 3), (mm2, REST0, 0), (rs1, 0, 0), (rs1n, 1, 0), (w_t, 2, 0),
        (mm1, OWN01, 8, 2), (w_t, 2, 1), (w_t, 2, 5), (act, OWN23, 2, 2), (rs2, 1, 0), (w_t, 2, 7), (rs2, 0, 0),
        (w_t, 2, 6), (w_t, 2, 2), (act, OWN23, 0, 1), (act, OWN01, 0, 1), (rs1n, 0, 0), (mm1, OWN01, 6, 2), (w_t, 2, 8),
        (mm1, FAR3, 0, 12), (mm2, REST1, 1), (act, REST2, 6, 6), (rs1, 1, 1), (mm2, REST0, 1), (rs1, 0, 1),
        (act, REST2, 0, 6), (mm2, REST2, 0), (rs1, 2, 0), (mm2, REST2, 1), (rs1n, 0, 1), (rs2, 1, 1), (rs1, 2, 1),
        (mm1, OWN01, 4, 2), (rs2, 0, 1), (mm1, NEAR3, 0, 6), (mm1, NEAR3, 6, 6), (rs1n, 1, 1), (mm1, OWN23Z1, 4, 8),
        (rs1n, 2, 0), (act, OWN01, 10, 2), (act, OWN01, 6, 2), (act, FAR3, 0, 12), (mm2, FAR3, 1), (mm2, FAR3, 0),
        (rs1, 3, 1), (rs1, 3, 0), (act, OWN01, 4, 2), (mm1, OWN23Z0, 8, 4), (act, OWN01, 8, 2), (rs2, 2, 1),
        (mm1, OWN23Z0, 4, 4), (rs1n, 2, 1), (mm2, OWN01, 0), (rs3, 0, 0), (rs3, 1, 0), (act, OWN23, 1, 1), (rs2, 2, 0),
        (mm2, OWN01, 1), (rs3, 0, 1), (rs3, 1, 1), (rs4, 0, 0), (act, NEAR3, 0, 6), (act, NEAR3, 6, 6), (mm2, NEAR3, 1),
        (rs1n, 3, 1), (rs2, 3, 1), (rs4, 1, 0), (mm2, NEAR3, 0), (rs4, 0, 1), (act, OWN23Z1, 4, 8), (rs1n, 3, 0),
        (mm2, OWN23Z1, 1), (rs2, 3, 0), (rs4, 1, 1), (rs3, 2, 1), (rs3, 3, 1), (mm2, OWN23Z1, 0), (act, OWN23Z0, 8, 4),
        (act, OWN23Z0, 4, 4), (rs3, 2, 0), (rs3, 3, 0), (mm2, OWN23Z0, 1), (rs4, 3, 1), (rs4, 2, 1), (mm2, OWN23Z0, 0),
        (rs4, 2, 0), (rs4, 3, 0),
    ]
    for copy in [load_tok] + vectors:
        copy.wait()
    for q in range(NQ):
        norm(q)
    pl.semaphore_wait(barrier, len(DEV))
    send_weights()
    for step, *args in order:
        step(*args)
    need(("f",))
    pltpu.make_async_copy(fr, fr, local_sems.at[3]).wait()
    wide = {n: C1 * sum(count for _, count, split_in in W1_CHUNKS if split_in == n) for n in (2, 4)}
    for group, ref in (
        ("a2a", nb), ("ag", x.at[pl.ds(0, 2)]), ("agf", x.at[FAR]), ("agz", x.at[OWN, :, 1]), ("b2", b2_far),
        ((1, 2), w1.at[pl.ds(0, kb), pl.ds(0, wide[2])]), ((1, 4), w1.at[pl.ds(0, kb), pl.ds(0, wide[4])]), ((2, 4), w2.at[1]),
        ("p", ps), ("r1", r1), ("r2", r2), ("rz", zs), ("f", fs),
    ):
        all_sent(group, ref)
    assert waited >= set(ids) and not groups
    assert len(ids) <= N_RECV, len(ids)


def local(tokens, ln_gain, w_in, b_in, w_out, b_out):
    n_tok, d = tokens.shape
    kb, nf = w_in.shape
    tq = n_tok // NQ
    pz = 2 * tq
    tiles = (4, NQ, 2, pz)
    vm = pltpu.VMEM
    flops = 4 * 16 * n_tok * 2 * kb * nf
    branch = pl.pallas_call(
        functools.partial(kernel, (tq, kb, nf)),
        out_shape=jax.ShapeDtypeStruct((n_tok, d), BF16),
        in_specs=[pl.BlockSpec(memory_space=pltpu.HBM)] * 6,
        out_specs=pl.BlockSpec(memory_space=pl.ANY),
        scratch_shapes=[
            vm((n_tok, d), BF16),
            vm((d,), F32),
            vm((nf,), F32),
            vm((kb,), F32),
            vm((2 * kb, nf), BF16),
            vm((2, nf, kb), BF16),
            vm(tiles + (2 * kb,), BF16),
            vm((n_tok, 2 * kb), BF16),
            vm(tiles + (nf,), F32),
            vm(tiles + (nf,), BF16),
            vm(tiles + (nf,), BF16),
            vm(tiles + (nf,), BF16),
            vm((2,) + tiles + (kb,), BF16),
            vm((2, NQ, 2, pz, kb), BF16),
            vm((2, NQ, 2, 2, pz, kb), BF16),
            vm((2, NQ, pz, kb), BF16),
            vm((2, NQ, pz, kb), BF16),
            vm((2, n_tok, kb), BF16),
            vm((2, n_tok, kb), BF16),
            vm((kb,), F32),
            pltpu.SemaphoreType.DMA((13,)),
            pltpu.SemaphoreType.DMA((N_RECV,)),
            pltpu.SemaphoreType.DMA((7,)),
        ],
        compiler_params=pltpu.CompilerParams(
            collective_id=0, has_side_effects=True, vmem_limit_bytes=52 * 2**20),
        cost_estimate=pl.CostEstimate(flops=flops, bytes_accessed=4 * kb * nf, transcendentals=0),
    )(*[pltpu.with_memory_space_constraint(a, pltpu.HBM) for a in (tokens, ln_gain, w_in, b_in, w_out, b_out)])
    return (tokens.astype(F32) + branch.astype(F32)).astype(BF16)


def solution(mesh):
    tokens = P(("grp", "row", "col"), None)
    return jax.shard_map(
        local,
        mesh=mesh,
        in_specs=(tokens, P(), P("row", "col"), P("col"), P("col", "row"), P("row")),
        out_specs=tokens,
        check_vma=False,
    )
```

```python
import functools

import jax
import jax.numpy as jnp
from jax import lax
from jax.experimental import pallas as pl
from jax.experimental.pallas import tpu as pltpu
from jax.sharding import PartitionSpec as P

MESH = pl.DeviceIdType.MESH
F32, BF16 = jnp.float32, jnp.bfloat16
NQ = 4
N_RECV = 158
SQRT_HALF = 0.7071067811865476
OWN, UP, DOWN, FAR = 0, 1, 2, 3
C1 = 128
W1_CHUNKS = ((0, 2, 4), (2, 2, 2), (4, 2, 4), (6, 2, 2), (8, 2, 4), (10, 2, 4))
NW2 = 9
Z = (0, 2)
OWN01, NEAR0, FAR0 = ((0, 1), (0, 2), Z), ((1, 3), (0, 1), Z), ((3, 4), (0, 1), Z)
REST0, REST1, REST2 = ((1, 4), (0, 1), Z), ((1, 4), (1, 2), Z), ((1, 4), (2, 3), Z)
NEAR3Z1, NEAR3Z0, FAR3 = ((1, 3), (3, 4), (1, 2)), ((1, 3), (3, 4), (0, 1)), ((3, 4), (3, 4), Z)
OWN23, OWN23Z1, OWN23Z0 = ((0, 1), (2, 4), Z), ((0, 1), (2, 4), (1, 2)), ((0, 1), (2, 4), (0, 1))


def kernel(dims, tok_hbm, gain_hbm, w1_hbm, b1_hbm, w2_hbm, b2_hbm, out,
           tok, gain, b1, b2_own, w1, w2, x, nb, p32, ps, pr, hid, os_, r1, r2, rf, zs, zr, fs, fr, b2_far,
           send_sems, recv_sems, local_sems):
    tq, kb, nf = dims
    nx = 4
    width = nx * kb

    grp, y, col = lax.axis_index("grp"), lax.axis_index("row"), lax.axis_index("col")
    xx, z, core, half = col // 2, col % 2, grp % 2, grp // 2
    m = y % 2
    y_pair = y + 1 - 2 * m
    y_far = 3 - y
    x_up, x_dn = (xx + 1) % 4, (xx + 3) % 4
    core_grp = grp + 1 - 2 * core
    twin_grp = grp + 2 - 4 * half
    diag_grp = core_grp + 2 - 4 * half
    DEV = {
        "pair": (grp, y_pair, col),
        "far": (grp, y_far, col),
        "core": (core_grp, y, col),
        "twin": (twin_grp, y, col),
        "up": (grp, y, x_up * 2 + z),
        "dn": (grp, y, x_dn * 2 + z),
        "z": (grp, y, xx * 2 + 1 - z),
    }
    my_blocks = (y, y_far)
    pair_blocks = (y_pair, 3 - y_pair)

    def lanes(block):
        return pl.ds(pl.multiple_of(block * kb, 128), kb)

    ids, landing, waited, groups = {}, {}, set(), {}

    def send(key, src, dst, to, landed=None, group=None):
        i = ids.setdefault(key, len(ids))
        g = groups.setdefault(group or key[0], len(groups))
        landing[key] = (dst if landed is None else landed, to, i)
        pltpu.make_async_remote_copy(
            src_ref=src, dst_ref=dst, send_sem=send_sems.at[g], recv_sem=recv_sems.at[i],
            device_id=DEV[to], device_id_type=MESH).start()

    def need(*keys):
        for key in keys:
            if key not in waited:
                waited.add(key)
                ref, to, i = landing[key]
                pltpu.make_async_remote_copy(
                    src_ref=ref, dst_ref=ref, send_sem=send_sems.at[0], recv_sem=recv_sems.at[i],
                    device_id=DEV[to], device_id_type=MESH).wait_recv()

    def all_sent(group, ref):
        pltpu.make_async_remote_copy(
            src_ref=ref, dst_ref=ref, send_sem=send_sems.at[groups.pop(group)], recv_sem=recv_sems.at[0],
            device_id=DEV["pair"], device_id_type=MESH).wait_send()

    load_tok = pltpu.make_async_copy(tok_hbm, tok, local_sems.at[2])
    load_tok.start()
    vectors = [
        pltpu.make_async_copy(src, dst, local_sems.at[4 + i])
        for i, (src, dst) in enumerate(((gain_hbm, gain), (b1_hbm, b1), (b2_hbm, b2_own)))]
    for copy in vectors:
        copy.start()
    load1 = pltpu.make_async_copy(w1_hbm, w1.at[pl.ds(0, kb)], local_sems.at[0])
    load1.start()
    barrier = pltpu.get_barrier_semaphore()
    for to in DEV:
        pl.semaphore_signal(barrier, inc=1, device_id=DEV[to], device_id_type=MESH)

    C2 = kb // 3
    load2 = pltpu.make_async_copy(w2_hbm, w2.at[0], local_sems.at[1])
    CHUNKS = [(1, c) for c in range(len(W1_CHUNKS))] + [(2, c) for c in range(NW2)]

    def split(which, c):
        return W1_CHUNKS[c][2] if which == 1 else 4

    def part(which, c, ref, owner_grp, base=0):
        n = split(which, c)
        owner = owner_grp if n == 4 else owner_grp % 2
        if which == 1:
            c0, width1, _ = W1_CHUNKS[c]
            size, cols = kb // n, pl.ds(c0 * C1, width1 * C1)
        else:
            size, cols = nf // n, pl.ds(c * (kb // NW2), kb // NW2)
        return ref.at[pl.ds(pl.multiple_of(base + owner * size, 32), size), cols]

    def far_part(which, c, owner):
        return part(which, c, w1, owner, kb) if which == 1 else part(which, c, w2.at[1], owner)

    def send_weights():
        for which, c in CHUNKS:
            src = part(which, c, w1_hbm if which == 1 else w2_hbm, grp)
            send(("wy", which, c), src, far_part(which, c, grp), "far", group=(which, split(which, c)))
        send(("b2",), b2_hbm, b2_far, "far")
        load2.start()

    def w_y(which, c):
        mine = far_part(which, c, grp)
        group = (which, split(which, c))
        need(("wy", which, c))
        if group[1] == 4:
            send(("wt", which, c), mine, mine, "twin", far_part(which, c, twin_grp), group)
        send(("wc", which, c), mine, mine, "core", far_part(which, c, core_grp), group)

    def w_t(which, c):
        theirs = far_part(which, c, twin_grp)
        need(("wt", which, c))
        send(("wd", which, c), theirs, theirs, "core", far_part(which, c, diag_grp), (which, 4))

    def w_all(which, c):
        need(("wy", which, c), ("wc", which, c))
        if split(which, c) == 4:
            need(("wt", which, c), ("wd", which, c))

    def half_rows(mi):
        return pl.ds(pl.multiple_of(mi * tq, tq), tq)

    def norm(q):
        rows = pl.ds(q * tq, tq)
        total = jnp.zeros((tq, 1), F32)
        for b in range(nx):
            total += jnp.sum(tok[rows, pl.ds(b * kb, kb)].astype(F32), axis=1, keepdims=True)
        mean = total / width
        sq = jnp.zeros((tq, 1), F32)
        for b in range(nx):
            d = tok[rows, pl.ds(b * kb, kb)].astype(F32) - mean
            sq += jnp.sum(d * d, axis=1, keepdims=True)
        scale = lax.rsqrt(sq / width + 1e-06)

        def normed(block):
            g = gain[lanes(block)].reshape(1, kb)
            return ((tok[rows, lanes(block)].astype(F32) - mean) * scale * g).astype(BF16)

        for i, block in enumerate(pair_blocks):
            nb[rows, pl.ds(i * kb, kb)] = normed(block)
        for i, block in enumerate(my_blocks):
            x[OWN, q, 0, half_rows(m), pl.ds(i * kb, kb)] = normed(block)

    def ag_y(q):
        there = x.at[OWN, q, 0, half_rows(m)]
        send(("a2a", q), nb.at[pl.ds(q * tq, tq)], there, "pair", x.at[OWN, q, 0, half_rows(1 - m)])

    def ag_rows(q, r):
        send(("agu0", q), x.at[OWN, q, 0, r], x.at[DOWN, q, 0, r], "up", x.at[DOWN, q, 0], "ag")
        send(("agd0", q), x.at[OWN, q, 0, r], x.at[UP, q, 0, r], "dn", x.at[UP, q, 0], "ag")

    def ag_x00(q):
        ag_rows(q, half_rows(m))

    def ag_z(q):
        need(("a2a", q))
        send(("agz", q), x.at[OWN, q, 0], x.at[OWN, q, 1], "z")

    def ag_x0(q):
        need(("a2a", q))
        ag_rows(q, half_rows(1 - m))

    def ag_x1(q):
        need(("agz", q))
        send(("agu1", q), x.at[OWN, q, 1], x.at[DOWN, q, 1], "up", group="ag")
        send(("agd1", q), x.at[OWN, q, 1], x.at[UP, q, 1], "dn", group="ag")

    def ag_fu(q):
        need(("agu0", q))
        send(("agf", q), x.at[DOWN, q, 0], x.at[FAR, q, 0], "up", x.at[FAR, q])

    def ag_fd(q):
        need(("agd1", q))
        send(("agf", q), x.at[UP, q, 1], x.at[FAR, q, 1], "dn", x.at[FAR, q])

    SOURCES = {
        (OWN, 0): "a2a", (OWN, 1): "agz", (UP, 0): "agd0", (UP, 1): "agd1",
        (DOWN, 0): "agu0", (DOWN, 1): "agu1", (FAR, 0): "agf", (FAR, 1): "agf",
    }

    def at(ref, unit, cols):
        (xa, xb), (qa, qb), (za, zb) = unit
        return ref.at[pl.ds(xa, xb - xa), pl.ds(qa, qb - qa), pl.ds(za, zb - za), :, cols]

    def blocks(unit):
        (xa, xb), (qa, qb), (za, zb) = unit
        return [(i, j, k) for i in range(xa, xb) for j in range(qa, qb) for k in range(za, zb)]

    def shape_of(unit):
        (xa, xb), (qa, qb), (za, zb) = unit
        return (xb - xa, qb - qa, zb - za, 2 * tq)

    def flat(ref, unit):
        v = at(ref, unit, slice(None))[...]
        return v.reshape(-1, v.shape[-1])

    def mm1(unit, c0, n):
        if not waited & {"w1"}:
            waited.add("w1")
            load1.wait()
        for i, j, k in blocks(unit):
            need((SOURCES[i, k], j))
        for c, (first, count, _) in enumerate(W1_CHUNKS):
            if first < c0 + n and c0 < first + count:
                w_all(1, c)
        wide = C1 * (2 - n % 2)

        @pl.loop(0, n * C1 // wide)
        def _(c):
            cols = pl.ds(pl.multiple_of(c0 * C1 + c * wide, C1), wide)
            acc = jnp.dot(flat(x, unit), w1[:, cols], preferred_element_type=F32)
            acc = acc.reshape(shape_of(unit) + (wide,))
            at(p32, unit, cols)[...] = acc
            at(ps, unit, cols)[...] = acc.astype(BF16)

        cols = pl.ds(c0 * C1, n * C1)
        send(("p", unit, c0), at(ps, unit, cols), at(pr, unit, cols), "pair")

    def act(unit, c0, n):
        need(("p", unit, c0))

        @pl.loop(c0, c0 + n)
        def _(c):
            cols = pl.ds(pl.multiple_of(c * C1, C1), C1)
            bias = b1[cols].reshape(1, C1)
            for i, j, k in blocks(unit):
                v = p32[i, j, k, :, cols] + pr[i, j, k, :, cols].astype(F32) + bias
                hid[i, j, k, :, cols] = (0.5 * v * (1.0 + lax.erf(v * SQRT_HALF))).astype(BF16)

    def mm2(unit, h):
        if not waited & {"w2"}:
            waited.add("w2")
            load2.wait()
        if h:
            for c in range(NW2):
                w_all(2, c)

        @pl.loop(0, 3)
        def _(c):
            cols = pl.ds(pl.multiple_of(c * C2, 128), C2)
            acc = jnp.dot(flat(hid, unit), w2[h, :, cols], preferred_element_type=F32)
            at(os_.at[h], unit, cols)[...] = acc.reshape(shape_of(unit) + (C2,)).astype(BF16)

    def add_to(ref, more):
        ref[...] = (ref[...].astype(F32) + more.astype(F32)).astype(BF16)

    def r2_send(q, h, d, z_pos):
        src = os_.at[h, UP + d, q, z_pos]
        send(("r2", q, h, z_pos), src, r2.at[h, q, z_pos, d], ("up", "dn")[d], r2.at[h, q, z_pos])

    def rsz(q, h):
        send(("rf", q, h), os_.at[h, FAR, q, 1], rf.at[h, q], "z")

    def rs1(q, h):
        need(("rf", q, h))
        add_to(os_.at[h, FAR, q, 0], rf[h, q])
        send(("r1", q, h), os_.at[h, FAR, q, 0], r1.at[h, q], ("up", "dn")[q % 2])

    def rs1n(q, h):
        d = q % 2
        r2_send(q, h, d, 1)
        r2_send(q, h, 1 - d, 1)

    def rs1o(q, h):
        r2_send(q, h, 1 - q % 2, 0)

    def rs2(q, h):
        d = q % 2
        need(("r1", q, h))
        add_to(os_.at[h, UP + d, q, 0], r1[h, q])
        r2_send(q, h, d, 0)

    def rs3(q, h):
        need(("r2", q, h, 1))
        s = os_[h, OWN, q, 1].astype(F32) + r2[h, q, 1, 0].astype(F32) + r2[h, q, 1, 1].astype(F32)
        zs[h, q] = s.astype(BF16)
        send(("rz", q, h), zs.at[h, q], zr.at[h, q], "z")

    def rs4(q, h):
        rows = pl.ds(q * tq, tq)
        need(("r2", q, h, 0), ("rz", q, h))
        if h:
            need(("b2",))
        bias = (b2_far if h else b2_own)[...].reshape(1, kb)

        def branch(mi):
            r = half_rows(mi)
            s = os_[h, OWN, q, 0, r].astype(F32) + r2[h, q, 0, 0, r].astype(F32) + r2[h, q, 0, 1, r].astype(F32)
            return (s + zr[h, q, r].astype(F32) + bias).astype(BF16)

        fs[h, rows, :] = branch(1 - m)
        there = out.at[rows, lanes(my_blocks[h])]
        send(("f",), fs.at[h, rows], there, "pair", fs)
        fr[h, rows, :] = branch(m)
        pltpu.make_async_copy(fr.at[h, rows], there, local_sems.at[3]).start()

    order = [
        (ag_y, 0), (ag_x00, 2), (ag_y, 1), (ag_y, 3), (ag_z, 0), (ag_x00, 0), (ag_y, 2), (ag_x0, 0), (w_y, 1, 0), (ag_z, 1),
        (ag_x00, 1), (ag_x1, 0), (w_t, 1, 0), (ag_fu, 0), (ag_z, 2), (ag_x0, 1), (ag_z, 3), (ag_fd, 0), (ag_x1, 1),
        (w_y, 1, 1), (mm1, NEAR0, 0, 2), (w_y, 1, 2), (ag_x00, 3), (mm1, OWN01, 0, 2), (mm1, NEAR0, 2, 2), (ag_fu, 1),
        (mm1, FAR0, 2, 2), (mm1, OWN01, 2, 2), (mm1, OWN23, 0, 2), (mm1, OWN23, 2, 2), (w_y, 1, 3), (ag_fd, 1),
        (mm1, FAR0, 0, 2), (mm1, FAR0, 6, 2), (w_t, 1, 2), (ag_x1, 3), (ag_x1, 2), (w_y, 1, 4), (ag_x0, 3),
        (mm1, OWN01, 6, 2), (mm1, NEAR0, 6, 2), (ag_x0, 2), (mm1, REST1, 0, 4), (w_y, 1, 5), (w_t, 1, 4), (w_y, 2, 0),
        (mm1, REST1, 4, 4), (w_y, 2, 2), (w_t, 1, 5), (act, NEAR0, 2, 2), (mm1, NEAR0, 4, 2), (w_y, 2, 1),
        (mm1, FAR0, 8, 2), (ag_fu, 2), (ag_fd, 2), (w_y, 2, 3), (mm1, REST1, 8, 4), (mm1, NEAR0, 8, 2), (w_y, 2, 5),
        (act, FAR0, 6, 2), (ag_fu, 3), (ag_fd, 3), (mm1, FAR0, 10, 2), (w_y, 2, 4), (act, REST1, 4, 4), (mm1, NEAR0, 10, 2),
        (act, REST1, 0, 4), (mm1, FAR0, 4, 2), (mm1, REST2, 6, 6), (w_y, 2, 6), (mm1, REST2, 0, 6), (act, REST1, 8, 4),
        (w_y, 2, 7), (mm1, FAR3, 0, 12), (w_y, 2, 8), (w_t, 2, 1), (act, NEAR0, 0, 2), (act, OWN01, 6, 2), (w_t, 2, 0),
        (act, FAR0, 10, 2), (w_t, 2, 3), (mm2, REST1, 0), (act, NEAR0, 8, 2), (act, FAR0, 2, 2), (mm1, OWN01, 8, 2),
        (w_t, 2, 4), (w_t, 2, 6), (act, NEAR0, 6, 2), (w_t, 2, 5), (act, OWN01, 0, 2), (rs1n, 1, 0), (act, FAR0, 0, 2),
        (rsz, 1, 0), (act, NEAR0, 4, 2), (act, FAR0, 4, 2), (act, OWN01, 2, 2), (act, FAR0, 8, 2), (mm1, OWN01, 10, 2),
        (w_t, 2, 2), (act, NEAR0, 10, 2), (mm2, REST0, 0), (rs1n, 0, 0), (mm1, OWN01, 4, 2), (w_t, 2, 7), (w_t, 2, 8),
        (rsz, 0, 0), (mm1, NEAR3Z1, 0, 12), (rs1o, 1, 0), (rs1, 1, 0), (mm2, REST0, 1), (rs1n, 0, 1), (rs1o, 0, 1),
        (rs1, 0, 0), (rsz, 0, 1), (mm1, OWN23Z1, 4, 8), (mm2, REST1, 1), (rs1o, 0, 0), (rsz, 1, 1), (act, REST2, 6, 6),
        (mm1, NEAR3Z0, 6, 6), (rs1n, 1, 1), (act, REST2, 0, 6), (mm2, REST2, 0), (rs1, 0, 1), (rs1o, 1, 1), (rsz, 2, 0),
        (mm2, REST2, 1), (rs1n, 2, 0), (act, FAR3, 0, 12), (rsz, 2, 1), (rs1, 1, 1), (mm2, FAR3, 0), (rsz, 3, 0),
        (act, OWN01, 8, 2), (rs2, 1, 0), (rs1n, 2, 1), (act, OWN23, 0, 2), (mm1, NEAR3Z0, 0, 6), (rs2, 0, 0),
        (act, OWN23, 2, 2), (mm2, FAR3, 1), (rs1, 2, 0), (rsz, 3, 1), (act, OWN01, 10, 2), (rs1, 2, 1), (rs2, 0, 1),
        (rs1o, 2, 0), (act, OWN01, 4, 2), (mm2, OWN01, 0), (rs3, 1, 0), (rs3, 0, 0), (mm2, OWN01, 1), (rs2, 1, 1),
        (rs3, 1, 1), (mm1, OWN23Z0, 4, 4), (mm1, OWN23Z0, 8, 4), (rs3, 0, 1), (act, NEAR3Z1, 0, 12), (rs1, 3, 1),
        (mm2, NEAR3Z1, 0), (rs1n, 3, 0), (rs4, 1, 0), (mm2, NEAR3Z1, 1), (rs4, 0, 0), (rs1, 3, 0), (rs2, 2, 0),
        (act, OWN23Z1, 4, 8), (rs1n, 3, 1), (mm2, OWN23Z1, 1), (rs4, 1, 1), (rs3, 2, 1), (rs2, 2, 1), (rs1o, 2, 1),
        (mm2, OWN23Z1, 0), (act, NEAR3Z0, 6, 6), (rs4, 0, 1), (rs3, 2, 0), (rs3, 3, 0), (act, NEAR3Z0, 0, 6),
        (mm2, NEAR3Z0, 0), (rs2, 3, 0), (rs1o, 3, 0), (mm2, NEAR3Z0, 1), (act, OWN23Z0, 4, 4), (rs3, 3, 1), (rs1o, 3, 1),
        (rs2, 3, 1), (act, OWN23Z0, 8, 4), (mm2, OWN23Z0, 1), (rs4, 2, 1), (mm2, OWN23Z0, 0), (rs4, 2, 0), (rs4, 3, 0),
        (rs4, 3, 1),
    ]
    for copy in [load_tok] + vectors:
        copy.wait()
    for q in range(NQ):
        norm(q)
    pl.semaphore_wait(barrier, len(DEV))
    send_weights()
    for step, *args in order:
        step(*args)
    need(("f",))
    pltpu.make_async_copy(fr, fr, local_sems.at[3]).wait()
    wide = {n: C1 * sum(count for _, count, split_in in W1_CHUNKS if split_in == n) for n in (2, 4)}
    for group, ref in (
        ("a2a", nb), ("ag", x.at[pl.ds(0, 2)]), ("agf", x.at[FAR]), ("agz", x.at[OWN, :, 1]), ("b2", b2_far),
        ((1, 2), w1.at[pl.ds(0, kb), pl.ds(0, wide[2])]), ((1, 4), w1.at[pl.ds(0, kb), pl.ds(0, wide[4])]), ((2, 4), w2.at[1]),
        ("p", ps), ("r1", r1), ("r2", r2), ("rf", rf), ("rz", zs), ("f", fs),
    ):
        all_sent(group, ref)
    assert waited >= set(ids) and not groups
    assert len(ids) <= N_RECV, len(ids)


def local(tokens, ln_gain, w_in, b_in, w_out, b_out):
    n_tok, d = tokens.shape
    kb, nf = w_in.shape
    tq = n_tok // NQ
    pz = 2 * tq
    tiles = (4, NQ, 2, pz)
    vm = pltpu.VMEM
    flops = 4 * 16 * n_tok * 2 * kb * nf
    branch = pl.pallas_call(
        functools.partial(kernel, (tq, kb, nf)),
        out_shape=jax.ShapeDtypeStruct((n_tok, d), BF16),
        in_specs=[pl.BlockSpec(memory_space=pltpu.HBM)] * 6,
        out_specs=pl.BlockSpec(memory_space=pl.ANY),
        scratch_shapes=[
            vm((n_tok, d), BF16),
            vm((d,), F32),
            vm((nf,), F32),
            vm((kb,), F32),
            vm((2 * kb, nf), BF16),
            vm((2, nf, kb), BF16),
            vm(tiles + (2 * kb,), BF16),
            vm((n_tok, 2 * kb), BF16),
            vm(tiles + (nf,), F32),
            vm(tiles + (nf,), BF16),
            vm(tiles + (nf,), BF16),
            vm(tiles + (nf,), BF16),
            vm((2,) + tiles + (kb,), BF16),
            vm((2, NQ, pz, kb), BF16),
            vm((2, NQ, 2, 2, pz, kb), BF16),
            vm((2, NQ, pz, kb), BF16),
            vm((2, NQ, pz, kb), BF16),
            vm((2, NQ, pz, kb), BF16),
            vm((2, n_tok, kb), BF16),
            vm((2, n_tok, kb), BF16),
            vm((kb,), F32),
            pltpu.SemaphoreType.DMA((14,)),
            pltpu.SemaphoreType.DMA((N_RECV,)),
            pltpu.SemaphoreType.DMA((7,)),
        ],
        compiler_params=pltpu.CompilerParams(
            collective_id=0, has_side_effects=True, vmem_limit_bytes=52 * 2**20),
        cost_estimate=pl.CostEstimate(flops=flops, bytes_accessed=4 * kb * nf, transcendentals=0),
    )(*[pltpu.with_memory_space_constraint(a, pltpu.HBM) for a in (tokens, ln_gain, w_in, b_in, w_out, b_out)])
    return (tokens.astype(F32) + branch.astype(F32)).astype(BF16)


def solution(mesh):
    tokens = P(("grp", "row", "col"), None)
    return jax.shard_map(
        local,
        mesh=mesh,
        in_specs=(tokens, P(), P("row", "col"), P("col"), P("col", "row"), P("row")),
        out_specs=tokens,
        check_vma=False,
    )
```

```python
import functools

import jax
import jax.numpy as jnp
from jax import lax
from jax.experimental import pallas as pl
from jax.experimental.pallas import tpu as pltpu
from jax.sharding import PartitionSpec as P

MESH = pl.DeviceIdType.MESH
F32, BF16 = jnp.float32, jnp.bfloat16
NQ = 4
N_RECV = 158
SQRT_HALF = 0.7071067811865476
OWN, UP, DOWN, FAR = 0, 1, 2, 3
C1 = 128
W1_CHUNKS = ((0, 2, 4), (2, 2, 2), (4, 2, 4), (6, 2, 2), (8, 2, 4), (10, 2, 4))
NW2 = 9
Z = (0, 2)
OWN01, NEAR0, FAR0 = ((0, 1), (0, 2), Z), ((1, 3), (0, 1), Z), ((3, 4), (0, 1), Z)
REST0, REST1, REST2 = ((1, 4), (0, 1), Z), ((1, 4), (1, 2), Z), ((1, 4), (2, 3), Z)
NEAR3Z1, NEAR3Z0, FAR3 = ((1, 3), (3, 4), (1, 2)), ((1, 3), (3, 4), (0, 1)), ((3, 4), (3, 4), Z)
OWN23, OWN23Z1, OWN23Z0 = ((0, 1), (2, 4), Z), ((0, 1), (2, 4), (1, 2)), ((0, 1), (2, 4), (0, 1))


def kernel(dims, tok_hbm, gain_hbm, w1_hbm, b1_hbm, w2_hbm, b2_hbm, out,
           tok, gain, b1, b2_own, w1, w2, x, nb, p32, ps, pr, hid, os_, r1, r2, rf, zs, zr, fs, fr, b2_far,
           send_sems, recv_sems, local_sems):
    tq, kb, nf = dims
    nx = 4
    width = nx * kb

    grp, y, col = lax.axis_index("grp"), lax.axis_index("row"), lax.axis_index("col")
    xx, z, core, half = col // 2, col % 2, grp % 2, grp // 2
    m = y % 2
    y_pair = y + 1 - 2 * m
    y_far = 3 - y
    x_up, x_dn = (xx + 1) % 4, (xx + 3) % 4
    core_grp = grp + 1 - 2 * core
    twin_grp = grp + 2 - 4 * half
    diag_grp = core_grp + 2 - 4 * half
    DEV = {
        "pair": (grp, y_pair, col),
        "far": (grp, y_far, col),
        "core": (core_grp, y, col),
        "twin": (twin_grp, y, col),
        "up": (grp, y, x_up * 2 + z),
        "dn": (grp, y, x_dn * 2 + z),
        "z": (grp, y, xx * 2 + 1 - z),
    }
    my_blocks = (y, y_far)
    pair_blocks = (y_pair, 3 - y_pair)

    def lanes(block):
        return pl.ds(pl.multiple_of(block * kb, 128), kb)

    ids, landing, waited, groups = {}, {}, set(), {}

    def send(key, src, dst, to, landed=None, group=None):
        i = ids.setdefault(key, len(ids))
        g = groups.setdefault(group or key[0], len(groups))
        landing[key] = (dst if landed is None else landed, to, i)
        pltpu.make_async_remote_copy(
            src_ref=src, dst_ref=dst, send_sem=send_sems.at[g], recv_sem=recv_sems.at[i],
            device_id=DEV[to], device_id_type=MESH).start()

    def need(*keys):
        for key in keys:
            if key not in waited:
                waited.add(key)
                ref, to, i = landing[key]
                pltpu.make_async_remote_copy(
                    src_ref=ref, dst_ref=ref, send_sem=send_sems.at[0], recv_sem=recv_sems.at[i],
                    device_id=DEV[to], device_id_type=MESH).wait_recv()

    def all_sent(group, ref):
        pltpu.make_async_remote_copy(
            src_ref=ref, dst_ref=ref, send_sem=send_sems.at[groups.pop(group)], recv_sem=recv_sems.at[0],
            device_id=DEV["pair"], device_id_type=MESH).wait_send()

    load_tok = pltpu.make_async_copy(tok_hbm, tok, local_sems.at[2])
    load_tok.start()
    vectors = [
        pltpu.make_async_copy(src, dst, local_sems.at[4 + i])
        for i, (src, dst) in enumerate(((gain_hbm, gain), (b1_hbm, b1), (b2_hbm, b2_own)))]
    for copy in vectors:
        copy.start()
    load1 = pltpu.make_async_copy(w1_hbm, w1.at[pl.ds(0, kb)], local_sems.at[0])
    load1.start()
    barrier = pltpu.get_barrier_semaphore()
    for to in DEV:
        pl.semaphore_signal(barrier, inc=1, device_id=DEV[to], device_id_type=MESH)

    C2 = kb // 3
    load2 = pltpu.make_async_copy(w2_hbm, w2.at[0], local_sems.at[1])
    CHUNKS = [(1, c) for c in range(len(W1_CHUNKS))] + [(2, c) for c in range(NW2)]

    def split(which, c):
        return W1_CHUNKS[c][2] if which == 1 else 4

    def part(which, c, ref, owner_grp, base=0):
        n = split(which, c)
        owner = owner_grp if n == 4 else owner_grp % 2
        if which == 1:
            c0, width1, _ = W1_CHUNKS[c]
            size, cols = kb // n, pl.ds(c0 * C1, width1 * C1)
        else:
            size, cols = nf // n, pl.ds(c * (kb // NW2), kb // NW2)
        return ref.at[pl.ds(pl.multiple_of(base + owner * size, 32), size), cols]

    def far_part(which, c, owner):
        return part(which, c, w1, owner, kb) if which == 1 else part(which, c, w2.at[1], owner)

    def send_weights():
        for which, c in CHUNKS:
            src = part(which, c, w1_hbm if which == 1 else w2_hbm, grp)
            send(("wy", which, c), src, far_part(which, c, grp), "far", group=(which, split(which, c)))
        send(("b2",), b2_hbm, b2_far, "far")
        load2.start()

    def w_y(which, c):
        mine = far_part(which, c, grp)
        group = (which, split(which, c))
        need(("wy", which, c))
        if group[1] == 4:
            send(("wt", which, c), mine, mine, "twin", far_part(which, c, twin_grp), group)
        send(("wc", which, c), mine, mine, "core", far_part(which, c, core_grp), group)

    def w_t(which, c):
        theirs = far_part(which, c, twin_grp)
        need(("wt", which, c))
        send(("wd", which, c), theirs, theirs, "core", far_part(which, c, diag_grp), (which, 4))

    def w_all(which, c):
        need(("wy", which, c), ("wc", which, c))
        if split(which, c) == 4:
            need(("wt", which, c), ("wd", which, c))

    def half_rows(mi):
        return pl.ds(pl.multiple_of(mi * tq, tq), tq)

    def norm(q):
        rows = pl.ds(q * tq, tq)
        total = jnp.zeros((tq, 1), F32)
        for b in range(nx):
            total += jnp.sum(tok[rows, pl.ds(b * kb, kb)].astype(F32), axis=1, keepdims=True)
        mean = total / width
        sq = jnp.zeros((tq, 1), F32)
        for b in range(nx):
            d = tok[rows, pl.ds(b * kb, kb)].astype(F32) - mean
            sq += jnp.sum(d * d, axis=1, keepdims=True)
        scale = lax.rsqrt(sq / width + 1e-06)

        def normed(block):
            g = gain[lanes(block)].reshape(1, kb)
            return ((tok[rows, lanes(block)].astype(F32) - mean) * scale * g).astype(BF16)

        for i, block in enumerate(pair_blocks):
            nb[rows, pl.ds(i * kb, kb)] = normed(block)
        for i, block in enumerate(my_blocks):
            x[OWN, q, 0, half_rows(m), pl.ds(i * kb, kb)] = normed(block)

    def ag_y(q):
        there = x.at[OWN, q, 0, half_rows(m)]
        send(("a2a", q), nb.at[pl.ds(q * tq, tq)], there, "pair", x.at[OWN, q, 0, half_rows(1 - m)])

    def ag_rows(q, r):
        send(("agu0", q), x.at[OWN, q, 0, r], x.at[DOWN, q, 0, r], "up", x.at[DOWN, q, 0], "ag")
        send(("agd0", q), x.at[OWN, q, 0, r], x.at[UP, q, 0, r], "dn", x.at[UP, q, 0], "ag")

    def ag_x00(q):
        ag_rows(q, half_rows(m))

    def ag_z(q):
        need(("a2a", q))
        send(("agz", q), x.at[OWN, q, 0], x.at[OWN, q, 1], "z")

    def ag_x0(q):
        need(("a2a", q))
        ag_rows(q, half_rows(1 - m))

    def ag_x1(q):
        need(("agz", q))
        send(("agu1", q), x.at[OWN, q, 1], x.at[DOWN, q, 1], "up", group="ag")
        send(("agd1", q), x.at[OWN, q, 1], x.at[UP, q, 1], "dn", group="ag")

    def ag_fu(q):
        need(("agu0", q))
        send(("agf", q), x.at[DOWN, q, 0], x.at[FAR, q, 0], "up", x.at[FAR, q])

    def ag_fd(q):
        need(("agd1", q))
        send(("agf", q), x.at[UP, q, 1], x.at[FAR, q, 1], "dn", x.at[FAR, q])

    SOURCES = {
        (OWN, 0): "a2a", (OWN, 1): "agz", (UP, 0): "agd0", (UP, 1): "agd1",
        (DOWN, 0): "agu0", (DOWN, 1): "agu1", (FAR, 0): "agf", (FAR, 1): "agf",
    }

    def at(ref, unit, cols):
        (xa, xb), (qa, qb), (za, zb) = unit
        return ref.at[pl.ds(xa, xb - xa), pl.ds(qa, qb - qa), pl.ds(za, zb - za), :, cols]

    def blocks(unit):
        (xa, xb), (qa, qb), (za, zb) = unit
        return [(i, j, k) for i in range(xa, xb) for j in range(qa, qb) for k in range(za, zb)]

    def shape_of(unit):
        (xa, xb), (qa, qb), (za, zb) = unit
        return (xb - xa, qb - qa, zb - za, 2 * tq)

    def flat(ref, unit):
        v = at(ref, unit, slice(None))[...]
        return v.reshape(-1, v.shape[-1])

    def mm1(unit, c0, n):
        if not waited & {"w1"}:
            waited.add("w1")
            load1.wait()
        for i, j, k in blocks(unit):
            need((SOURCES[i, k], j))
        for c, (first, count, _) in enumerate(W1_CHUNKS):
            if first < c0 + n and c0 < first + count:
                w_all(1, c)
        wide = C1 * (2 - n % 2)

        @pl.loop(0, n * C1 // wide)
        def _(c):
            cols = pl.ds(pl.multiple_of(c0 * C1 + c * wide, C1), wide)
            acc = jnp.dot(flat(x, unit), w1[:, cols], preferred_element_type=F32)
            acc = acc.reshape(shape_of(unit) + (wide,))
            at(p32, unit, cols)[...] = acc
            at(ps, unit, cols)[...] = acc.astype(BF16)

        cols = pl.ds(c0 * C1, n * C1)
        send(("p", unit, c0), at(ps, unit, cols), at(pr, unit, cols), "pair")

    def act(unit, c0, n):
        need(("p", unit, c0))

        @pl.loop(c0, c0 + n)
        def _(c):
            cols = pl.ds(pl.multiple_of(c * C1, C1), C1)
            bias = b1[cols].reshape(1, C1)
            for i, j, k in blocks(unit):
                v = p32[i, j, k, :, cols] + pr[i, j, k, :, cols].astype(F32) + bias
                hid[i, j, k, :, cols] = (0.5 * v * (1.0 + lax.erf(v * SQRT_HALF))).astype(BF16)

    def mm2(unit, h):
        if not waited & {"w2"}:
            waited.add("w2")
            load2.wait()
        if h:
            for c in range(NW2):
                w_all(2, c)

        @pl.loop(0, 3)
        def _(c):
            cols = pl.ds(pl.multiple_of(c * C2, 128), C2)
            acc = jnp.dot(flat(hid, unit), w2[h, :, cols], preferred_element_type=F32)
            at(os_.at[h], unit, cols)[...] = acc.reshape(shape_of(unit) + (C2,)).astype(BF16)

    def add_to(ref, more):
        ref[...] = (ref[...].astype(F32) + more.astype(F32)).astype(BF16)

    def r2_send(q, h, d, z_pos):
        src = os_.at[h, UP + d, q, z_pos]
        send(("r2", q, h, z_pos), src, r2.at[h, q, z_pos, d], ("up", "dn")[d], r2.at[h, q, z_pos])

    def rsz(q, h):
        send(("rf", q, h), os_.at[h, FAR, q, 1], rf.at[h, q], "z")

    def rs1(q, h):
        need(("rf", q, h))
        add_to(os_.at[h, FAR, q, 0], rf[h, q])
        send(("r1", q, h), os_.at[h, FAR, q, 0], r1.at[h, q], ("up", "dn")[q % 2])

    def rs1n(q, h):
        d = q % 2
        r2_send(q, h, d, 1)
        r2_send(q, h, 1 - d, 1)

    def rs1o(q, h):
        r2_send(q, h, 1 - q % 2, 0)

    def rs2(q, h):
        d = q % 2
        need(("r1", q, h))
        add_to(os_.at[h, UP + d, q, 0], r1[h, q])
        r2_send(q, h, d, 0)

    def rs3(q, h):
        need(("r2", q, h, 1))
        s = os_[h, OWN, q, 1].astype(F32) + r2[h, q, 1, 0].astype(F32) + r2[h, q, 1, 1].astype(F32)
        zs[h, q] = s.astype(BF16)
        send(("rz", q, h), zs.at[h, q], zr.at[h, q], "z")

    def rs4(q, h):
        rows = pl.ds(q * tq, tq)
        need(("r2", q, h, 0), ("rz", q, h))
        if h:
            need(("b2",))
        bias = (b2_far if h else b2_own)[...].reshape(1, kb)

        def branch(mi):
            r = half_rows(mi)
            s = os_[h, OWN, q, 0, r].astype(F32) + r2[h, q, 0, 0, r].astype(F32) + r2[h, q, 0, 1, r].astype(F32)
            return (s + zr[h, q, r].astype(F32) + bias).astype(BF16)

        fs[h, rows, :] = branch(1 - m)
        there = out.at[rows, lanes(my_blocks[h])]
        send(("f",), fs.at[h, rows], there, "pair", fs)
        fr[h, rows, :] = branch(m)
        pltpu.make_async_copy(fr.at[h, rows], there, local_sems.at[3]).start()

    order = [
        (ag_y, 0), (ag_y, 1), (ag_x00, 0), (ag_y, 3), (ag_y, 2), (ag_x00, 3), (ag_z, 0), (w_y, 1, 0), (ag_z, 1), (ag_z, 3),
        (ag_x00, 1), (ag_z, 2), (ag_x0, 0), (ag_x1, 0), (w_y, 1, 1), (ag_x0, 1), (w_t, 1, 0), (ag_x1, 1),
        (mm1, OWN01, 2, 2), (ag_fd, 0), (w_y, 1, 2), (mm1, OWN01, 0, 2), (mm1, NEAR0, 2, 2), (ag_fu, 0), (mm1, NEAR0, 0, 2),
        (ag_fd, 1), (mm1, OWN23, 0, 2), (ag_fu, 1), (w_y, 1, 3), (ag_x00, 2), (mm1, OWN23, 2, 2), (mm1, FAR0, 0, 2),
        (ag_x0, 2), (mm1, FAR0, 2, 2), (w_y, 1, 4), (w_t, 1, 2), (mm1, FAR0, 6, 2), (mm1, NEAR0, 6, 2), (ag_x1, 2),
        (mm1, OWN01, 6, 2), (w_y, 1, 5), (mm1, REST1, 0, 4), (ag_x0, 3), (w_y, 2, 0), (w_t, 1, 4), (w_y, 2, 1),
        (mm1, REST1, 4, 4), (w_y, 2, 2), (ag_x1, 3), (act, NEAR0, 6, 2), (w_t, 1, 5), (w_y, 2, 3), (mm1, NEAR0, 8, 2),
        (mm1, NEAR0, 4, 2), (ag_fu, 2), (act, NEAR0, 0, 2), (ag_fu, 3), (mm1, FAR0, 4, 2), (mm1, FAR0, 8, 2),
        (act, NEAR0, 2, 2), (ag_fd, 2), (mm1, REST1, 8, 4), (w_y, 2, 5), (ag_fd, 3), (mm1, FAR0, 10, 2), (act, OWN01, 2, 2),
        (act, REST1, 4, 4), (w_y, 2, 6), (mm1, NEAR0, 10, 2), (w_y, 2, 4), (mm1, REST2, 6, 6), (w_y, 2, 7),
        (act, REST1, 0, 4), (mm1, REST2, 0, 6), (act, OWN23, 0, 2), (w_y, 2, 8), (mm1, FAR3, 0, 12), (act, REST1, 8, 4),
        (w_t, 2, 0), (mm2, REST1, 0), (w_t, 2, 2), (act, FAR0, 10, 2), (act, FAR0, 4, 2), (act, NEAR0, 8, 2), (w_t, 2, 1),
        (mm1, OWN01, 8, 2), (act, FAR0, 2, 2), (act, NEAR0, 10, 2), (act, OWN01, 6, 2), (mm1, OWN01, 4, 2), (w_t, 2, 6),
        (act, NEAR0, 4, 2), (act, OWN01, 0, 2), (act, FAR0, 8, 2), (w_t, 2, 5), (rsz, 1, 0), (w_t, 2, 3), (w_t, 2, 7),
        (act, FAR0, 6, 2), (rs1n, 1, 0), (act, FAR0, 0, 2), (mm2, REST0, 0), (w_t, 2, 4), (rs1n, 0, 0), (rs1o, 0, 0),
        (act, OWN23, 2, 2), (rs1o, 1, 0), (w_t, 2, 8), (mm1, OWN01, 10, 2), (rsz, 0, 0), (mm1, NEAR3Z1, 0, 12),
        (mm2, REST1, 1), (rsz, 1, 1), (rs1, 0, 0), (act, REST2, 6, 6), (rs1n, 1, 1), (mm2, REST0, 1), (rs1, 1, 0),
        (rs1o, 0, 1), (rsz, 0, 1), (mm1, OWN23Z1, 4, 8), (mm1, NEAR3Z0, 6, 6), (rs1n, 0, 1), (rs1, 1, 1), (rs2, 0, 0),
        (act, REST2, 0, 6), (mm2, REST2, 0), (rs1n, 2, 0), (mm2, REST2, 1), (rs1o, 1, 1), (mm1, NEAR3Z0, 0, 6),
        (rs1o, 2, 1), (rs1, 0, 1), (rsz, 2, 1), (act, FAR3, 0, 12), (mm2, FAR3, 0), (rsz, 2, 0), (rs2, 1, 1),
        (mm2, FAR3, 1), (rsz, 3, 1), (rsz, 3, 0), (rs2, 1, 0), (rs1n, 2, 1), (mm1, OWN23Z0, 8, 4), (mm1, OWN23Z0, 4, 4),
        (rs1, 2, 1), (act, OWN01, 4, 2), (act, OWN01, 8, 2), (act, OWN01, 10, 2), (rs1o, 2, 0), (mm2, OWN01, 1),
        (rs1, 2, 0), (rs3, 1, 1), (mm2, OWN01, 0), (rs3, 0, 0), (rs2, 0, 1), (act, NEAR3Z1, 0, 12), (rs3, 1, 0),
        (rs1, 3, 1), (mm2, NEAR3Z1, 1), (rs2, 2, 1), (rs1, 3, 0), (mm2, NEAR3Z1, 0), (rs1n, 3, 0), (act, OWN23Z1, 4, 8),
        (rs1n, 3, 1), (rs4, 1, 1), (rs3, 0, 1), (mm2, OWN23Z1, 1), (rs2, 2, 0), (rs3, 2, 1), (rs4, 0, 0), (mm2, OWN23Z1, 0),
        (rs4, 1, 0), (rs3, 2, 0), (act, NEAR3Z0, 6, 6), (act, NEAR3Z0, 0, 6), (mm2, NEAR3Z0, 0), (rs1o, 3, 0), (rs3, 3, 0),
        (rs2, 3, 0), (rs4, 0, 1), (mm2, NEAR3Z0, 1), (rs1o, 3, 1), (act, OWN23Z0, 8, 4), (rs2, 3, 1), (rs3, 3, 1),
        (act, OWN23Z0, 4, 4), (mm2, OWN23Z0, 0), (rs4, 2, 0), (mm2, OWN23Z0, 1), (rs4, 2, 1), (rs4, 3, 0), (rs4, 3, 1),
    ]
    for copy in [load_tok] + vectors:
        copy.wait()
    for q in range(NQ):
        norm(q)
    pl.semaphore_wait(barrier, len(DEV))
    send_weights()
    for step, *args in order:
        step(*args)
    need(("f",))
    pltpu.make_async_copy(fr, fr, local_sems.at[3]).wait()
    wide = {n: C1 * sum(count for _, count, split_in in W1_CHUNKS if split_in == n) for n in (2, 4)}
    for group, ref in (
        ("a2a", nb), ("ag", x.at[pl.ds(0, 2)]), ("agf", x.at[FAR]), ("agz", x.at[OWN, :, 1]), ("b2", b2_far),
        ((1, 2), w1.at[pl.ds(0, kb), pl.ds(0, wide[2])]), ((1, 4), w1.at[pl.ds(0, kb), pl.ds(0, wide[4])]), ((2, 4), w2.at[1]),
        ("p", ps), ("r1", r1), ("r2", r2), ("rf", rf), ("rz", zs), ("f", fs),
    ):
        all_sent(group, ref)
    assert waited >= set(ids) and not groups
    assert len(ids) <= N_RECV, len(ids)


def local(tokens, ln_gain, w_in, b_in, w_out, b_out):
    n_tok, d = tokens.shape
    kb, nf = w_in.shape
    tq = n_tok // NQ
    pz = 2 * tq
    tiles = (4, NQ, 2, pz)
    vm = pltpu.VMEM
    flops = 4 * 16 * n_tok * 2 * kb * nf
    branch = pl.pallas_call(
        functools.partial(kernel, (tq, kb, nf)),
        out_shape=jax.ShapeDtypeStruct((n_tok, d), BF16),
        in_specs=[pl.BlockSpec(memory_space=pltpu.HBM)] * 6,
        out_specs=pl.BlockSpec(memory_space=pl.ANY),
        scratch_shapes=[
            vm((n_tok, d), BF16),
            vm((d,), F32),
            vm((nf,), F32),
            vm((kb,), F32),
            vm((2 * kb, nf), BF16),
            vm((2, nf, kb), BF16),
            vm(tiles + (2 * kb,), BF16),
            vm((n_tok, 2 * kb), BF16),
            vm(tiles + (nf,), F32),
            vm(tiles + (nf,), BF16),
            vm(tiles + (nf,), BF16),
            vm(tiles + (nf,), BF16),
            vm((2,) + tiles + (kb,), BF16),
            vm((2, NQ, pz, kb), BF16),
            vm((2, NQ, 2, 2, pz, kb), BF16),
            vm((2, NQ, pz, kb), BF16),
            vm((2, NQ, pz, kb), BF16),
            vm((2, NQ, pz, kb), BF16),
            vm((2, n_tok, kb), BF16),
            vm((2, n_tok, kb), BF16),
            vm((kb,), F32),
            pltpu.SemaphoreType.DMA((14,)),
            pltpu.SemaphoreType.DMA((N_RECV,)),
            pltpu.SemaphoreType.DMA((7,)),
        ],
        compiler_params=pltpu.CompilerParams(
            collective_id=0, has_side_effects=True, vmem_limit_bytes=52 * 2**20),
        cost_estimate=pl.CostEstimate(flops=flops, bytes_accessed=4 * kb * nf, transcendentals=0),
    )(*[pltpu.with_memory_space_constraint(a, pltpu.HBM) for a in (tokens, ln_gain, w_in, b_in, w_out, b_out)])
    return (tokens.astype(F32) + branch.astype(F32)).astype(BF16)


def solution(mesh):
    tokens = P(("grp", "row", "col"), None)
    return jax.shard_map(
        local,
        mesh=mesh,
        in_specs=(tokens, P(), P("row", "col"), P("col"), P("col", "row"), P("row")),
        out_specs=tokens,
        check_vma=False,
    )
```

```python
import functools

import jax
import jax.numpy as jnp
from jax import lax
from jax.experimental import pallas as pl
from jax.experimental.pallas import tpu as pltpu
from jax.sharding import PartitionSpec as P

MESH = pl.DeviceIdType.MESH
F32, BF16 = jnp.float32, jnp.bfloat16
NQ = 4
N_RECV = 156
SQRT_HALF = 0.7071067811865476
OWN, UP, DOWN, FAR = 0, 1, 2, 3
C1 = 128
W1_CHUNKS = ((0, 2, 4), (2, 2, 2), (4, 2, 4), (6, 2, 2), (8, 2, 4), (10, 2, 2))
NW2 = 9
Z = (0, 2)
OWN01, NEAR0, FAR0 = ((0, 1), (0, 2), Z), ((1, 3), (0, 1), Z), ((3, 4), (0, 1), Z)
REST0, REST1, REST2 = ((1, 4), (0, 1), Z), ((1, 4), (1, 2), Z), ((1, 4), (2, 3), Z)
NEAR3Z1, NEAR3Z0, FAR3 = ((1, 3), (3, 4), (1, 2)), ((1, 3), (3, 4), (0, 1)), ((3, 4), (3, 4), Z)
OWN23, OWN23Z1, OWN23Z0 = ((0, 1), (2, 4), Z), ((0, 1), (2, 4), (1, 2)), ((0, 1), (2, 4), (0, 1))


def kernel(dims, tok_hbm, gain_hbm, w1_hbm, b1_hbm, w2_hbm, b2_hbm, out,
           tok, gain, b1, b2_own, w1, w2, x, nb, p32, ps, pr, hid, os_, r1, r2, rf, zs, zr, fs, fr, b2_far,
           send_sems, recv_sems, local_sems):
    tq, kb, nf = dims
    nx = 4
    width = nx * kb

    grp, y, col = lax.axis_index("grp"), lax.axis_index("row"), lax.axis_index("col")
    xx, z, core, half = col // 2, col % 2, grp % 2, grp // 2
    m = y % 2
    y_pair = y + 1 - 2 * m
    y_far = 3 - y
    x_up, x_dn = (xx + 1) % 4, (xx + 3) % 4
    core_grp = grp + 1 - 2 * core
    twin_grp = grp + 2 - 4 * half
    diag_grp = core_grp + 2 - 4 * half
    DEV = {
        "pair": (grp, y_pair, col),
        "far": (grp, y_far, col),
        "core": (core_grp, y, col),
        "twin": (twin_grp, y, col),
        "up": (grp, y, x_up * 2 + z),
        "dn": (grp, y, x_dn * 2 + z),
        "z": (grp, y, xx * 2 + 1 - z),
    }
    my_blocks = (y, y_far)
    pair_blocks = (y_pair, 3 - y_pair)

    def lanes(block):
        return pl.ds(pl.multiple_of(block * kb, 128), kb)

    ids, landing, waited, groups = {}, {}, set(), {}

    def send(key, src, dst, to, landed=None, group=None):
        i = ids.setdefault(key, len(ids))
        g = groups.setdefault(group or key[0], len(groups))
        landing[key] = (dst if landed is None else landed, to, i)
        pltpu.make_async_remote_copy(
            src_ref=src, dst_ref=dst, send_sem=send_sems.at[g], recv_sem=recv_sems.at[i],
            device_id=DEV[to], device_id_type=MESH).start()

    def need(*keys):
        for key in keys:
            if key not in waited:
                waited.add(key)
                ref, to, i = landing[key]
                pltpu.make_async_remote_copy(
                    src_ref=ref, dst_ref=ref, send_sem=send_sems.at[0], recv_sem=recv_sems.at[i],
                    device_id=DEV[to], device_id_type=MESH).wait_recv()

    def all_sent(group, ref):
        pltpu.make_async_remote_copy(
            src_ref=ref, dst_ref=ref, send_sem=send_sems.at[groups.pop(group)], recv_sem=recv_sems.at[0],
            device_id=DEV["pair"], device_id_type=MESH).wait_send()

    load_tok = pltpu.make_async_copy(tok_hbm, tok, local_sems.at[2])
    load_tok.start()
    vectors = [
        pltpu.make_async_copy(src, dst, local_sems.at[4 + i])
        for i, (src, dst) in enumerate(((gain_hbm, gain), (b1_hbm, b1), (b2_hbm, b2_own)))]
    for copy in vectors:
        copy.start()
    load1 = pltpu.make_async_copy(w1_hbm, w1.at[pl.ds(0, kb)], local_sems.at[0])
    load1.start()
    barrier = pltpu.get_barrier_semaphore()
    for to in DEV:
        pl.semaphore_signal(barrier, inc=1, device_id=DEV[to], device_id_type=MESH)

    C2 = kb // 3
    load2 = pltpu.make_async_copy(w2_hbm, w2.at[0], local_sems.at[1])
    CHUNKS = [(1, c) for c in range(len(W1_CHUNKS))] + [(2, c) for c in range(NW2)]

    def split(which, c):
        return W1_CHUNKS[c][2] if which == 1 else 4

    def part(which, c, ref, owner_grp, base=0):
        n = split(which, c)
        owner = owner_grp if n == 4 else owner_grp % 2
        if which == 1:
            c0, width1, _ = W1_CHUNKS[c]
            size, cols = kb // n, pl.ds(c0 * C1, width1 * C1)
        else:
            size, cols = nf // n, pl.ds(c * (kb // NW2), kb // NW2)
        return ref.at[pl.ds(pl.multiple_of(base + owner * size, 32), size), cols]

    def far_part(which, c, owner):
        return part(which, c, w1, owner, kb) if which == 1 else part(which, c, w2.at[1], owner)

    def send_weights():
        for which, c in CHUNKS:
            src = part(which, c, w1_hbm if which == 1 else w2_hbm, grp)
            send(("wy", which, c), src, far_part(which, c, grp), "far", group=(which, split(which, c)))
        send(("b2",), b2_hbm, b2_far, "far")
        load2.start()

    def w_y(which, c):
        mine = far_part(which, c, grp)
        group = (which, split(which, c))
        need(("wy", which, c))
        if group[1] == 4:
            send(("wt", which, c), mine, mine, "twin", far_part(which, c, twin_grp), group)
        send(("wc", which, c), mine, mine, "core", far_part(which, c, core_grp), group)

    def w_t(which, c):
        theirs = far_part(which, c, twin_grp)
        need(("wt", which, c))
        send(("wd", which, c), theirs, theirs, "core", far_part(which, c, diag_grp), (which, 4))

    def w_all(which, c):
        need(("wy", which, c), ("wc", which, c))
        if split(which, c) == 4:
            need(("wt", which, c), ("wd", which, c))

    def half_rows(mi):
        return pl.ds(pl.multiple_of(mi * tq, tq), tq)

    def norm(q):
        rows = pl.ds(q * tq, tq)
        total = jnp.zeros((tq, 1), F32)
        for b in range(nx):
            total += jnp.sum(tok[rows, pl.ds(b * kb, kb)].astype(F32), axis=1, keepdims=True)
        mean = total / width
        sq = jnp.zeros((tq, 1), F32)
        for b in range(nx):
            d = tok[rows, pl.ds(b * kb, kb)].astype(F32) - mean
            sq += jnp.sum(d * d, axis=1, keepdims=True)
        scale = lax.rsqrt(sq / width + 1e-06)

        def normed(block):
            g = gain[lanes(block)].reshape(1, kb)
            return ((tok[rows, lanes(block)].astype(F32) - mean) * scale * g).astype(BF16)

        for i, block in enumerate(pair_blocks):
            nb[rows, pl.ds(i * kb, kb)] = normed(block)
        for i, block in enumerate(my_blocks):
            x[OWN, q, 0, half_rows(m), pl.ds(i * kb, kb)] = normed(block)

    def ag_y(q):
        there = x.at[OWN, q, 0, half_rows(m)]
        send(("a2a", q), nb.at[pl.ds(q * tq, tq)], there, "pair", x.at[OWN, q, 0, half_rows(1 - m)])

    def ag_rows(q, r):
        send(("agu0", q), x.at[OWN, q, 0, r], x.at[DOWN, q, 0, r], "up", x.at[DOWN, q, 0], "ag")
        send(("agd0", q), x.at[OWN, q, 0, r], x.at[UP, q, 0, r], "dn", x.at[UP, q, 0], "ag")

    def ag_x00(q):
        ag_rows(q, half_rows(m))

    def ag_z(q):
        need(("a2a", q))
        send(("agz", q), x.at[OWN, q, 0], x.at[OWN, q, 1], "z")

    def ag_x0(q):
        need(("a2a", q))
        ag_rows(q, half_rows(1 - m))

    def ag_x1(q):
        need(("agz", q))
        send(("agu1", q), x.at[OWN, q, 1], x.at[DOWN, q, 1], "up", group="ag")
        send(("agd1", q), x.at[OWN, q, 1], x.at[UP, q, 1], "dn", group="ag")

    def ag_fu(q):
        need(("agu0", q))
        send(("agf", q), x.at[DOWN, q, 0], x.at[FAR, q, 0], "up", x.at[FAR, q])

    def ag_fd(q):
        need(("agd1", q))
        send(("agf", q), x.at[UP, q, 1], x.at[FAR, q, 1], "dn", x.at[FAR, q])

    SOURCES = {
        (OWN, 0): "a2a", (OWN, 1): "agz", (UP, 0): "agd0", (UP, 1): "agd1",
        (DOWN, 0): "agu0", (DOWN, 1): "agu1", (FAR, 0): "agf", (FAR, 1): "agf",
    }

    def at(ref, unit, cols):
        (xa, xb), (qa, qb), (za, zb) = unit
        return ref.at[pl.ds(xa, xb - xa), pl.ds(qa, qb - qa), pl.ds(za, zb - za), :, cols]

    def blocks(unit):
        (xa, xb), (qa, qb), (za, zb) = unit
        return [(i, j, k) for i in range(xa, xb) for j in range(qa, qb) for k in range(za, zb)]

    def shape_of(unit):
        (xa, xb), (qa, qb), (za, zb) = unit
        return (xb - xa, qb - qa, zb - za, 2 * tq)

    def flat(ref, unit):
        v = at(ref, unit, slice(None))[...]
        return v.reshape(-1, v.shape[-1])

    def mm1(unit, c0, n):
        if not waited & {"w1"}:
            waited.add("w1")
            load1.wait()
        for i, j, k in blocks(unit):
            need((SOURCES[i, k], j))
        for c, (first, count, _) in enumerate(W1_CHUNKS):
            if first < c0 + n and c0 < first + count:
                w_all(1, c)
        wide = C1 * (2 - n % 2)

        @pl.loop(0, n * C1 // wide)
        def _(c):
            cols = pl.ds(pl.multiple_of(c0 * C1 + c * wide, C1), wide)
            acc = jnp.dot(flat(x, unit), w1[:, cols], preferred_element_type=F32)
            acc = acc.reshape(shape_of(unit) + (wide,))
            at(p32, unit, cols)[...] = acc
            at(ps, unit, cols)[...] = acc.astype(BF16)

        cols = pl.ds(c0 * C1, n * C1)
        send(("p", unit, c0), at(ps, unit, cols), at(pr, unit, cols), "pair")

    def act(unit, c0, n):
        need(("p", unit, c0))

        @pl.loop(c0, c0 + n)
        def _(c):
            cols = pl.ds(pl.multiple_of(c * C1, C1), C1)
            bias = b1[cols].reshape(1, C1)
            for i, j, k in blocks(unit):
                v = p32[i, j, k, :, cols] + pr[i, j, k, :, cols].astype(F32) + bias
                hid[i, j, k, :, cols] = (0.5 * v * (1.0 + lax.erf(v * SQRT_HALF))).astype(BF16)

    def mm2(unit, h):
        if not waited & {"w2"}:
            waited.add("w2")
            load2.wait()
        if h:
            for c in range(NW2):
                w_all(2, c)

        @pl.loop(0, 3)
        def _(c):
            cols = pl.ds(pl.multiple_of(c * C2, 128), C2)
            acc = jnp.dot(flat(hid, unit), w2[h, :, cols], preferred_element_type=F32)
            at(os_.at[h], unit, cols)[...] = acc.reshape(shape_of(unit) + (C2,)).astype(BF16)

    def add_to(ref, more):
        ref[...] = (ref[...].astype(F32) + more.astype(F32)).astype(BF16)

    def r2_send(q, h, d, z_pos):
        src = os_.at[h, UP + d, q, z_pos]
        send(("r2", q, h, z_pos), src, r2.at[h, q, z_pos, d], ("up", "dn")[d], r2.at[h, q, z_pos])

    def rsz(q, h):
        send(("rf", q, h), os_.at[h, FAR, q, 1], rf.at[h, q], "z")

    def rs1(q, h):
        need(("rf", q, h))
        add_to(os_.at[h, FAR, q, 0], rf[h, q])
        send(("r1", q, h), os_.at[h, FAR, q, 0], r1.at[h, q], ("up", "dn")[q % 2])

    def rs1n(q, h):
        d = q % 2
        r2_send(q, h, d, 1)
        r2_send(q, h, 1 - d, 1)

    def rs1o(q, h):
        r2_send(q, h, 1 - q % 2, 0)

    def rs2(q, h):
        d = q % 2
        need(("r1", q, h))
        add_to(os_.at[h, UP + d, q, 0], r1[h, q])
        r2_send(q, h, d, 0)

    def rs3(q, h):
        need(("r2", q, h, 1))
        s = os_[h, OWN, q, 1].astype(F32) + r2[h, q, 1, 0].astype(F32) + r2[h, q, 1, 1].astype(F32)
        zs[h, q] = s.astype(BF16)
        send(("rz", q, h), zs.at[h, q], zr.at[h, q], "z")

    def rs4(q, h):
        rows = pl.ds(q * tq, tq)
        need(("r2", q, h, 0), ("rz", q, h))
        if h:
            need(("b2",))
        bias = (b2_far if h else b2_own)[...].reshape(1, kb)

        def branch(mi):
            r = half_rows(mi)
            s = os_[h, OWN, q, 0, r].astype(F32) + r2[h, q, 0, 0, r].astype(F32) + r2[h, q, 0, 1, r].astype(F32)
            return (s + zr[h, q, r].astype(F32) + bias).astype(BF16)

        fs[h, rows, :] = branch(1 - m)
        there = out.at[rows, lanes(my_blocks[h])]
        send(("f",), fs.at[h, rows], there, "pair", fs)
        fr[h, rows, :] = branch(m)
        pltpu.make_async_copy(fr.at[h, rows], there, local_sems.at[3]).start()

    order = [
        (ag_y, 0), (ag_x00, 3), (ag_x00, 0), (ag_z, 0), (ag_x0, 0), (ag_x00, 2), (ag_y, 3), (ag_x00, 1), (ag_y, 1),
        (w_y, 1, 0), (ag_x1, 0), (ag_y, 2), (ag_x0, 1), (ag_fu, 0), (ag_z, 1), (w_t, 1, 0), (ag_z, 2), (w_y, 1, 1),
        (ag_fd, 0), (ag_z, 3), (mm1, NEAR0, 0, 2), (mm1, NEAR0, 2, 2), (mm1, OWN01, 0, 2), (ag_x0, 2), (w_y, 1, 2),
        (ag_x1, 1), (mm1, OWN01, 2, 2), (mm1, FAR0, 0, 2), (mm1, FAR0, 2, 2), (mm1, OWN23, 2, 2), (ag_fu, 1), (w_y, 1, 3),
        (mm1, OWN23, 0, 2), (ag_fd, 1), (act, FAR0, 2, 2), (mm1, FAR0, 6, 2), (w_t, 1, 2), (ag_x1, 2), (mm1, NEAR0, 6, 2),
        (ag_x1, 3), (w_y, 1, 4), (mm1, OWN01, 6, 2), (mm1, NEAR0, 4, 2), (act, FAR0, 0, 2), (mm1, REST1, 0, 4), (w_t, 1, 4),
        (w_y, 1, 5), (mm1, REST1, 4, 4), (w_y, 2, 0), (act, OWN23, 0, 2), (ag_fu, 2), (act, NEAR0, 4, 2), (mm1, FAR0, 4, 2),
        (ag_x0, 3), (w_y, 2, 1), (act, OWN01, 0, 2), (mm1, REST1, 8, 4), (ag_fd, 2), (w_y, 2, 2), (act, NEAR0, 0, 2),
        (act, REST1, 0, 4), (ag_fd, 3), (mm1, FAR0, 8, 2), (mm1, NEAR0, 8, 2), (act, OWN01, 2, 2), (mm1, FAR0, 10, 2),
        (w_y, 2, 3), (mm1, NEAR0, 10, 2), (w_y, 2, 4), (ag_fu, 3), (w_y, 2, 5), (mm1, REST2, 6, 6), (w_t, 2, 0),
        (act, FAR0, 4, 2), (mm1, OWN01, 4, 2), (w_y, 2, 6), (mm1, REST2, 0, 6), (act, FAR0, 8, 2), (act, REST1, 8, 4),
        (w_t, 2, 2), (act, NEAR0, 2, 2), (act, FAR0, 6, 2), (mm1, OWN01, 8, 2), (w_y, 2, 7), (act, NEAR0, 8, 2),
        (act, REST1, 4, 4), (mm2, REST1, 0), (w_y, 2, 8), (act, NEAR0, 10, 2), (w_t, 2, 5), (act, FAR0, 10, 2),
        (act, NEAR0, 6, 2), (mm2, REST0, 0), (w_t, 2, 3), (rsz, 0, 0), (mm1, OWN01, 10, 2), (w_t, 2, 4), (w_t, 2, 1),
        (rs1o, 0, 0), (rsz, 1, 0), (rs1n, 0, 0), (rs1o, 1, 0), (mm1, FAR3, 0, 12), (rs1n, 1, 0), (w_t, 2, 6), (w_t, 2, 8),
        (w_t, 2, 7), (mm1, NEAR3Z1, 0, 12), (mm2, REST0, 1), (rs1, 0, 0), (rsz, 0, 1), (rs1n, 0, 1), (mm2, REST1, 1),
        (act, OWN01, 6, 2), (rs1, 1, 0), (act, REST2, 6, 6), (mm1, OWN23Z1, 4, 8), (rs1n, 1, 1), (rs1o, 1, 1), (rsz, 1, 1),
        (rs1o, 0, 1), (mm1, NEAR3Z0, 6, 6), (act, REST2, 0, 6), (mm2, REST2, 1), (rsz, 2, 1), (rs2, 1, 0), (rs1, 0, 1),
        (act, OWN23, 2, 2), (mm2, REST2, 0), (rs1, 1, 1), (rs1n, 2, 1), (rs1n, 2, 0), (act, OWN01, 8, 2),
        (act, OWN01, 4, 2), (rs2, 0, 0), (act, OWN01, 10, 2), (mm2, OWN01, 0), (rs3, 1, 0), (mm1, NEAR3Z0, 0, 6),
        (rsz, 2, 0), (mm1, OWN23Z0, 8, 4), (act, FAR3, 0, 12), (mm2, FAR3, 0), (rsz, 3, 0), (rs2, 0, 1), (rs1o, 2, 0),
        (mm1, OWN23Z0, 4, 4), (rs4, 1, 0), (rs2, 1, 1), (rs3, 0, 0), (mm2, FAR3, 1), (rs1, 2, 1), (rsz, 3, 1), (rs1, 2, 0),
        (mm2, OWN01, 1), (act, NEAR3Z1, 0, 12), (rs1, 3, 0), (rs3, 1, 1), (mm2, NEAR3Z1, 0), (rs1n, 3, 0), (rs4, 0, 0),
        (rs3, 0, 1), (mm2, NEAR3Z1, 1), (act, OWN23Z1, 4, 8), (rs1n, 3, 1), (mm2, OWN23Z1, 1), (rs3, 2, 1),
        (act, NEAR3Z0, 6, 6), (rs1, 3, 1), (rs2, 2, 1), (rs2, 2, 0), (rs4, 1, 1), (mm2, OWN23Z1, 0), (rs3, 2, 0),
        (rs1o, 2, 1), (act, NEAR3Z0, 0, 6), (rs4, 0, 1), (rs3, 3, 0), (mm2, NEAR3Z0, 0), (rs2, 3, 0), (rs1o, 3, 0),
        (mm2, NEAR3Z0, 1), (act, OWN23Z0, 8, 4), (rs2, 3, 1), (rs1o, 3, 1), (rs3, 3, 1), (act, OWN23Z0, 4, 4),
        (mm2, OWN23Z0, 0), (rs4, 2, 0), (mm2, OWN23Z0, 1), (rs4, 2, 1), (rs4, 3, 0), (rs4, 3, 1),
    ]
    for copy in [load_tok] + vectors:
        copy.wait()
    for q in range(NQ):
        norm(q)
    pl.semaphore_wait(barrier, len(DEV))
    send_weights()
    for step, *args in order:
        step(*args)
    need(("f",))
    pltpu.make_async_copy(fr, fr, local_sems.at[3]).wait()
    wide = {n: C1 * sum(count for _, count, split_in in W1_CHUNKS if split_in == n) for n in (2, 4)}
    for group, ref in (
        ("a2a", nb), ("ag", x.at[pl.ds(0, 2)]), ("agf", x.at[FAR]), ("agz", x.at[OWN, :, 1]), ("b2", b2_far),
        ((1, 2), w1.at[pl.ds(0, kb), pl.ds(0, wide[2])]), ((1, 4), w1.at[pl.ds(0, kb), pl.ds(0, wide[4])]), ((2, 4), w2.at[1]),
        ("p", ps), ("r1", r1), ("r2", r2), ("rf", rf), ("rz", zs), ("f", fs),
    ):
        all_sent(group, ref)
    assert waited >= set(ids) and not groups
    assert len(ids) <= N_RECV, len(ids)


def local(tokens, ln_gain, w_in, b_in, w_out, b_out):
    n_tok, d = tokens.shape
    kb, nf = w_in.shape
    tq = n_tok // NQ
    pz = 2 * tq
    tiles = (4, NQ, 2, pz)
    vm = pltpu.VMEM
    flops = 4 * 16 * n_tok * 2 * kb * nf
    branch = pl.pallas_call(
        functools.partial(kernel, (tq, kb, nf)),
        out_shape=jax.ShapeDtypeStruct((n_tok, d), BF16),
        in_specs=[pl.BlockSpec(memory_space=pltpu.HBM)] * 6,
        out_specs=pl.BlockSpec(memory_space=pl.ANY),
        scratch_shapes=[
            vm((n_tok, d), BF16),
            vm((d,), F32),
            vm((nf,), F32),
            vm((kb,), F32),
            vm((2 * kb, nf), BF16),
            vm((2, nf, kb), BF16),
            vm(tiles + (2 * kb,), BF16),
            vm((n_tok, 2 * kb), BF16),
            vm(tiles + (nf,), F32),
            vm(tiles + (nf,), BF16),
            vm(tiles + (nf,), BF16),
            vm(tiles + (nf,), BF16),
            vm((2,) + tiles + (kb,), BF16),
            vm((2, NQ, pz, kb), BF16),
            vm((2, NQ, 2, 2, pz, kb), BF16),
            vm((2, NQ, pz, kb), BF16),
            vm((2, NQ, pz, kb), BF16),
            vm((2, NQ, pz, kb), BF16),
            vm((2, n_tok, kb), BF16),
            vm((2, n_tok, kb), BF16),
            vm((kb,), F32),
            pltpu.SemaphoreType.DMA((14,)),
            pltpu.SemaphoreType.DMA((N_RECV,)),
            pltpu.SemaphoreType.DMA((7,)),
        ],
        compiler_params=pltpu.CompilerParams(
            collective_id=0, has_side_effects=True, vmem_limit_bytes=52 * 2**20),
        cost_estimate=pl.CostEstimate(flops=flops, bytes_accessed=4 * kb * nf, transcendentals=0),
    )(*[pltpu.with_memory_space_constraint(a, pltpu.HBM) for a in (tokens, ln_gain, w_in, b_in, w_out, b_out)])
    return (tokens.astype(F32) + branch.astype(F32)).astype(BF16)


def solution(mesh):
    tokens = P(("grp", "row", "col"), None)
    return jax.shard_map(
        local,
        mesh=mesh,
        in_specs=(tokens, P(), P("row", "col"), P("col"), P("col", "row"), P("row")),
        out_specs=tokens,
        check_vma=False,
    )
```
